128 devices in a mesh: node: 32 (over x, z, core), dev: 4 (over y).
Axes of the slice: x: 4, y: 4, z: 4, core: 2. Of those that a mesh axis runs over, the one named last changes fastest.
Arguments:
- kv_pages: bfloat16 [16384, 1, 2, 16, 1024], P(('node', 'dev')), may hold values from -6 to 6
- new_slot: int32 [16384], P(('node', 'dev')), may hold values from 0 to 16383, as said below
- request_rate: float32 [2048], P(('node', 'dev')), may hold values from 0.25 to 4
- page_table: int32 [2048, 128], P(('node', 'dev')), may hold values from 0 to 16383
Outputs:
- migrated: bfloat16 [16384, 1, 2, 16, 1024], P(('node', 'dev'))
- device_load: float32 [128], replicated
The draws below stay inside these ranges and needn't reach their ends.
Inputs may be any that keep to these rules, and one draw needn't show every extreme that they name: new_slot is a permutation of the slots; slot p lies on device p // 128. Every device sends exactly 127 of its pages to other devices, at most one to any one device, and receives exactly 127 into the slots that its leaving pages free; its other pages keep their slots.
All inputs are finite; a program needn't handle non-finite values.
Results may differ from the reference program's by a relative error of at most 0.001.
Values may be sent and summed in bfloat16 or wider, within the bound.
A program may use at most 128 MiB of HBM per device.

```python
import math
import jax
import jax.numpy as jnp
import numpy as np

KVH = 8
HD = 128
LAYERS = 1
PAGE_TOK = 16
PPR = 128
PAGE_DEV = 128
REQ_DEV = 16
MOVE_DEV = 127
PAGES = 16384
REQS = 2048
N_NODE = 32
N_DEV = 4


def freed_slots(one_key):
    return jax.random.permutation(one_key, PAGE_DEV)[:MOVE_DEV]


def draw_new_slot(key, part):
    device_total = N_NODE * N_DEV
    page_total = PAGE_DEV * device_total
    key_label, key_shift, key_slots = jax.random.split(jax.random.fold_in(key, 17), 3)
    relabel = jax.random.permutation(key_label, device_total).astype(jnp.int32)
    shifts = (jax.random.permutation(key_shift, device_total - 1)[:MOVE_DEV] + 1).astype(jnp.int32)
    slot_keys = jax.random.split(key_slots, device_total)
    freed = jax.vmap(freed_slots)(slot_keys).astype(jnp.int32)
    position = jnp.arange(device_total, dtype=jnp.int32)
    rounds = jnp.broadcast_to(jnp.arange(MOVE_DEV, dtype=jnp.int32)[None, :], (device_total, MOVE_DEV))
    senders = jnp.broadcast_to(relabel[:, None], (device_total, MOVE_DEV))
    takers = relabel[(position[:, None] + shifts[None, :]) % device_total]
    from_index = senders * PAGE_DEV + freed[senders, rounds]
    to_index = takers * PAGE_DEV + freed[takers, rounds]
    base = jnp.arange(page_total, dtype=jnp.int32)
    return base.at[from_index.reshape(-1)].set(to_index.reshape(-1))


def set_ends(array, own_key, least, top_value):
    longest = array.shape.index(max(array.shape))
    spots = []
    for shift in (0, 1):
        where = [jax.random.randint(jax.random.fold_in(own_key, axis), (), 0, length) for axis, length in enumerate(array.shape)]
        where[longest] = (where[longest] + shift) % array.shape[longest]
        spots.append(tuple(where))
    return array.at[spots[0]].set(least).at[spots[1]].set(top_value)


def shard_levels(stream_key, extent, pieces, low, top_value):
    gain, own = 1.0, jax.random.fold_in(stream_key, 6)
    for axis_at, shards_of in pieces:
        heights = jnp.exp(jax.random.uniform(jax.random.fold_in(own, axis_at), (shards_of,), jnp.float32, low / len(pieces), top_value / len(pieces)))
        gain = gain * jnp.repeat(heights, extent[axis_at] // shards_of).reshape([-1 if axis == axis_at else 1 for axis in range(len(extent))])
    return gain


def rank_bounds(number_of, skew):
    loads = [(1 << 20) // math.isqrt(grade ** skew) + 1 for grade in range(1, number_of + 1)]
    deviation = 1 + sum(loads) // (1 << 30)
    return np.cumsum(np.array([max(1, weight // deviation) for weight in loads]))


def skewed_ids(key, dims, number_of, lean):
    grid = rank_bounds(number_of, lean)
    ticket = jax.random.randint(jax.random.fold_in(key, 1), dims, 0, int(grid[number_of - 1]))
    standing = jnp.searchsorted(jnp.asarray(grid, jnp.int32), ticket, side="right")
    return jax.random.permutation(jax.random.fold_in(key, 2), number_of)[standing].astype(jnp.int32)


def normal_values(stream_key, extent, spread, most, pieces=(), kind=jnp.bfloat16):
    values = spread * jax.random.normal(stream_key, extent, jnp.float32)
    if pieces:
        values = values * shard_levels(stream_key, extent, pieces, -0.22, 0.18)
    return jnp.clip(values, -most, most).astype(kind)


def setup_inputs(seed: int = 0) -> dict:
    splits = jax.random.split(jax.random.key(seed), 5)
    return {
        "kv_pages": normal_values(splits[0], (PAGES, LAYERS, 2, PAGE_TOK, KVH * HD), 1.0, 6.0, ((0, 128),)),
        "new_slot": draw_new_slot(jax.random.fold_in(splits[4], 71), 0),
        "request_rate": jnp.clip(jnp.exp(math.log(4.0) - 2.7725887 * jax.random.uniform(splits[2], (REQS,), jnp.float32) ** shard_levels(splits[2], (REQS,), ((0, 128),), -0.2, 0.2)), 0.25, 4.0),
        "page_table": set_ends(skewed_ids(splits[3], (REQS, PPR), PAGES, 2), jax.random.fold_in(splits[3], 3), 0, PAGES - 1).astype(jnp.int32),
    }


def reference(kv_pages, new_slot, request_rate, page_table):
    page_total = kv_pages.shape[0]
    device_total = N_NODE * N_DEV
    source = jnp.zeros((page_total,), jnp.int32).at[new_slot].set(jnp.arange(page_total, dtype=jnp.int32))
    migrated = jnp.take(kv_pages, source, axis=0)
    weights = jnp.broadcast_to(request_rate[:, None], page_table.shape).reshape(-1)
    page_warmth = jnp.zeros((page_total,), jnp.float32).at[page_table.reshape(-1)].add(weights)
    owners = (new_slot // PAGE_DEV).astype(jnp.int32)
    summed = jax.ops.segment_sum(page_warmth, owners, num_segments=device_total)
    device_load = summed / (PPR * REQ_DEV)
    return migrated, device_load
```

```python
import jax
import jax.numpy as jnp
import numpy as np
from jax import lax
from jax.experimental import pallas as pl
from jax.experimental.pallas import tpu as pltpu
from jax.sharding import Mesh
from jax.sharding import PartitionSpec as P

AXES = ("x", "z", "c", "y")
SIZE = {"x": 4, "z": 4, "c": 2, "y": 4}
DEVICES = 128
ORDERS = (("x", "y", "z"), ("y", "z", "x"), ("z", "x", "y"))
LATE = (2, 1, 3, 0)
AWAY = (2, 1, 3)


def make_plan():
    keyed = []
    for rel in range(DEVICES):
        step = {"x": rel // 32, "z": rel // 8 % 4, "c": rel // 4 % 2, "y": rel % 4}
        group = sum(step.values()) % 3
        first, second, third = (step[a] for a in ORDERS[group])
        keyed.append((group, first, second, third, step["c"], rel))
    keyed.sort()
    place = np.zeros((DEVICES,), np.int32)
    chunks = {}
    for row, (group, first, second, third, core, rel) in enumerate(keyed):
        place[rel] = row
        chunks.setdefault((group, first, second), []).append((row, third, core))
    return place, chunks


PLACE, CHUNKS = make_plan()


def my_index():
    at = [lax.axis_index(a) for a in AXES]
    return ((at[0] * 4 + at[1]) * 2 + at[2]) * 4 + at[3]


def partner(**steps):
    return tuple(
        jnp.bitwise_xor(lax.axis_index(a), steps[a]) if steps.get(a) else lax.axis_index(a)
        for a in AXES
    )


def along(axis, step, core=0):
    return partner(**{axis: step, "c": core})


def pack_kernel(slot_ref, place_ref, pages_ref, out_ref, sem):
    me = my_index()

    @pl.loop(0, DEVICES)
    def _(p):
        row = place_ref[jnp.bitwise_xor(lax.shift_right_logical(slot_ref[p], 7), me)]
        pltpu.make_async_copy(pages_ref.at[p, 0], out_ref.at[row], sem).start()

    pltpu.make_async_copy(out_ref, out_ref, sem).wait()


def place_kernel(slot_ref, place_ref, total_ref, pages_ref, out_ref, load_ref, sem):
    me = my_index()

    @pl.loop(0, DEVICES)
    def _(e):
        row = place_ref[jnp.bitwise_xor(e, me)]
        pltpu.make_async_copy(pages_ref.at[row], out_ref.at[slot_ref[0, e], 0], sem).start()

    load_ref[...] = total_ref[...] * (1.0 / 2048.0)
    pltpu.make_async_copy(pages_ref, pages_ref, sem).wait()


def exchange_kernel(
    rate_ref, table_ref, slots_ref, send_ref,
    pages_ref, slot_out_ref, load_ref,
    mid1, mid2, known, row1, row2, row3, part1, part2, part3,
    sent, got1, got2, got3, local, small_sent, small_got,
):
    x, z, c, y = (lax.axis_index(a) for a in AXES)
    me = my_index()
    row = c * 4 + y
    remote = lambda src, dst, ss, rs, dev: pltpu.make_async_remote_copy(
        src, dst, ss, rs, device_id=dev, device_id_type=pl.DeviceIdType.MESH
    )

    def wait(ref, sem):
        pltpu.make_async_copy(ref, ref, sem).wait()

    keep = pltpu.make_async_copy(slots_ref, known.at[x, z, pl.ds(row, 1)], local.at[0])
    keep.start()
    barrier = pltpu.get_barrier_semaphore()
    peers = [partner(c=1)] + [along(a, s, k) for a in "xyz" for s in AWAY for k in (0, 1)]
    for dev in peers:
        pl.semaphore_signal(barrier, inc=1, device_id=dev, device_id_type=pl.DeviceIdType.MESH)
    pl.semaphore_wait(barrier, len(peers))

    cell = [partner(c=k, y=s) for k in (0, 1) for s in range(4) if k or s]

    def span(key):
        rows = CHUNKS[key]
        return pl.ds(rows[0][0], len(rows))

    def spot(key):
        return (key[0] * 4 + key[1]) * 4 + key[2]

    def source(key):
        return mid2 if key[2] else (mid1 if key[1] else send_ref)

    def phase1(key):
        remote(
            send_ref.at[span(key)], mid1.at[span(key)], sent.at[0], got1.at[spot(key)],
            along(ORDERS[key[0]][0], key[1]),
        ).start()

    def phase2(key):
        src = mid1 if key[1] else send_ref
        remote(
            src.at[span(key)], mid2.at[span(key)], sent.at[1], got2.at[spot(key)],
            along(ORDERS[key[0]][1], key[2]),
        ).start()

    def phase3(key):
        src = source(key)
        for page, step, core in CHUNKS[key]:
            if step or core:
                remote(
                    src.at[page], pages_ref.at[page], sent.at[2], got3,
                    along(ORDERS[key[0]][2], step, core),
                ).start()
            else:
                pltpu.make_async_copy(src.at[page], pages_ref.at[page], local.at[1]).start()

    def start1(second):
        for first in AWAY:
            for g in range(3):
                phase1((g, first, second))

    def forward2(second):
        for first in AWAY:
            for g in range(3):
                key = (g, first, second)
                wait(mid1.at[span(key)], got1.at[spot(key)])
                phase2(key)

    def tell(src, dst, k, devs):
        for dev in devs:
            remote(src, dst, small_sent.at[k], small_got.at[k], dev).start()

    zs = [partner(z=s) for s in AWAY]
    xs = [partner(x=s) for s in AWAY]

    tell(slots_ref, known.at[x, z, pl.ds(row, 1)], 0, cell)
    start1(2)
    keep.wait()
    wait(known.at[0, 0, pl.ds(0, 7)], small_got.at[0])
    tell(known.at[x, z], known.at[x, z], 1, zs)
    start1(1)
    wait(known.at[0, pl.ds(0, 3)], small_got.at[1])
    tell(known.at[x], known.at[x], 2, xs)
    start1(3)
    wait(known.at[pl.ds(0, 3)], small_got.at[2])
    start1(0)

    slots = known[...].reshape(DEVICES, DEVICES)
    owner = lax.shift_right_logical(slots, 7)
    owner_t = owner.astype(jnp.float32).T.astype(jnp.bfloat16)
    down = lax.broadcasted_iota(jnp.int32, (DEVICES, DEVICES), 0)

    def entry(r, acc):
        page = table_ref[pl.ds(r, 1), :]
        high = lax.shift_right_logical(page, 7)
        low = jnp.bitwise_and(page, 127)
        pick = jnp.where(down == high, 1.0, 0.0).astype(jnp.bfloat16)
        column = jnp.dot(owner_t, pick, preferred_element_type=jnp.float32)
        mine = jnp.sum(jnp.where(down == low, column, 0.0), axis=0, keepdims=True)
        return acc + jnp.where(down == mine.astype(jnp.int32), rate_ref[r], 0.0)

    acc = lax.fori_loop(0, 16, entry, jnp.zeros((DEVICES, DEVICES), jnp.float32))
    first_sum = jnp.sum(acc.T, axis=0, keepdims=True)
    part1[...] = first_sum
    row1[pl.ds(row, 1), :] = first_sum
    to_me = jnp.where(owner == me, jnp.bitwise_and(slots, 127), 0).astype(jnp.float32)
    slot_out_ref[...] = jnp.sum(to_me.T, axis=0, keepdims=True).astype(jnp.int32)

    tell(part1, row1.at[pl.ds(row, 1)], 3, cell)
    for second in AWAY:
        for g in range(3):
            phase2((g, 0, second))
    forward2(2)
    wait(row1.at[pl.ds(0, 7)], small_got.at[3])
    second_sum = jnp.sum(row1[...], axis=0, keepdims=True)
    part2[...] = second_sum
    row2[pl.ds(z, 1), :] = second_sum
    forward2(1)
    tell(part2, row2.at[pl.ds(z, 1)], 4, zs)
    forward2(3)
    wait(row2.at[pl.ds(0, 3)], small_got.at[4])
    third_sum = jnp.sum(row2[...], axis=0, keepdims=True)
    part3[...] = third_sum
    row3[pl.ds(x, 1), :] = third_sum
    for g in range(3):
        phase3((g, 0, 0))
    for first in AWAY:
        for g in range(3):
            key = (g, first, 0)
            wait(mid1.at[span(key)], got1.at[spot(key)])
            phase3(key)
    tell(part3, row3.at[pl.ds(x, 1)], 5, xs)
    for second in AWAY:
        for g in range(3):
            key = (g, 0, second)
            wait(mid2.at[span(key)], got2.at[spot(key)])
            phase3(key)
    for second in AWAY:
        for first in AWAY:
            for g in range(3):
                key = (g, first, second)
                wait(mid2.at[span(key)], got2.at[spot(key)])
                phase3(key)
    wait(row3.at[pl.ds(0, 3)], small_got.at[5])
    load_ref[...] = jnp.sum(row3[...], axis=0, keepdims=True)

    pages = [sum(len(v) for k, v in CHUNKS.items() if k[i]) for i in (1, 2)]
    far = sum(1 for v in CHUNKS.values() for _, s, k in v if s or k)
    wait(send_ref.at[pl.ds(0, pages[0])], sent.at[0])
    wait(send_ref.at[pl.ds(0, pages[1])], sent.at[1])
    wait(send_ref.at[pl.ds(0, far)], sent.at[2])
    wait(pages_ref.at[pl.ds(0, far)], got3)
    wait(pages_ref.at[pl.ds(0, DEVICES - far)], local.at[1])
    wait(known.at[0, 0, pl.ds(0, 7)], small_sent.at[0])
    wait(known.at[0, pl.ds(0, 3)], small_sent.at[1])
    wait(known.at[pl.ds(0, 3)], small_sent.at[2])
    wait(row1.at[pl.ds(0, 7)], small_sent.at[3])
    wait(row2.at[pl.ds(0, 3)], small_sent.at[4])
    wait(row3.at[pl.ds(0, 3)], small_sent.at[5])


SMEM = pl.BlockSpec(memory_space=pltpu.SMEM)
VMEM = pl.BlockSpec(memory_space=pltpu.VMEM)
HBM = pl.BlockSpec(memory_space=pltpu.HBM)


def on_device(kv_pages, new_slot, request_rate, page_table):
    block = jax.ShapeDtypeStruct((DEVICES,) + kv_pages.shape[2:], kv_pages.dtype)
    buffer = pltpu.VMEM(block.shape, block.dtype)
    line = lambda dtype: jax.ShapeDtypeStruct((1, DEVICES), dtype)
    place = jnp.asarray(PLACE)
    packed = pl.pallas_call(
        pack_kernel,
        out_shape=block,
        in_specs=[SMEM, SMEM, HBM],
        out_specs=VMEM,
        scratch_shapes=[pltpu.SemaphoreType.DMA],
        compiler_params=pltpu.CompilerParams(vmem_limit_bytes=45 << 20),
        name="pack",
    )(new_slot, place, kv_pages)
    row = lambda n, dtype=jnp.float32: pltpu.VMEM((n, DEVICES), dtype)
    dma = pltpu.SemaphoreType.DMA
    arrived, slot, total = pl.pallas_call(
        exchange_kernel,
        out_shape=(block, line(jnp.int32), line(jnp.float32)),
        in_specs=[SMEM, VMEM, VMEM, VMEM],
        out_specs=(VMEM, VMEM, VMEM),
        scratch_shapes=[
            buffer, buffer, pltpu.VMEM((4, 4, 8, DEVICES), jnp.int32),
            row(8), row(4), row(4), row(1), row(1), row(1),
            dma((3,)), dma((48,)), dma((48,)), dma, dma((2,)), dma((6,)), dma((6,)),
        ],
        compiler_params=pltpu.CompilerParams(
            collective_id=0, has_side_effects=True, vmem_limit_bytes=20 << 20
        ),
        name="exchange",
    )(request_rate, page_table, new_slot.reshape(1, DEVICES), packed)
    migrated, load = pl.pallas_call(
        place_kernel,
        out_shape=(jax.ShapeDtypeStruct(kv_pages.shape, kv_pages.dtype), line(jnp.float32)),
        in_specs=[SMEM, SMEM, VMEM, VMEM],
        out_specs=(HBM, VMEM),
        scratch_shapes=[dma],
        compiler_params=pltpu.CompilerParams(vmem_limit_bytes=12 << 20),
        name="place",
    )(slot, place, total, arrived)
    return migrated, load.reshape(DEVICES)


def solution(mesh):
    split = Mesh(mesh.devices.reshape(4, 4, 2, mesh.shape["dev"]), AXES)
    placed = (P(AXES, None, None, None, None), P(AXES), P(AXES), P(AXES, None))
    return jax.shard_map(
        on_device,
        mesh=split,
        in_specs=placed,
        out_specs=(P(AXES, None, None, None, None), P()),
        check_vma=False,
    )
```

```python
import jax
import jax.numpy as jnp
import numpy as np
from jax import lax
from jax.experimental import pallas as pl
from jax.experimental.pallas import tpu as pltpu
from jax.sharding import Mesh
from jax.sharding import PartitionSpec as P

AXES = ("x", "z", "c", "y")
SIZE = {"x": 4, "z": 4, "c": 2, "y": 4}
DEVICES = 128
ORDERS = (("x", "y", "z"), ("y", "z", "x"), ("z", "x", "y"))
LATE = (2, 1, 3, 0)
AWAY = (2, 1, 3)
LATE_SUM = 3


def make_plan():
    keyed = []
    for rel in range(DEVICES):
        step = {"x": rel // 32, "z": rel // 8 % 4, "c": rel // 4 % 2, "y": rel % 4}
        group = sum(step.values()) % 3
        first, second, third = (step[a] for a in ORDERS[group])
        keyed.append((group, first, second, third, step["c"], rel))
    keyed.sort()
    place = np.zeros((DEVICES,), np.int32)
    chunks = {}
    for row, (group, first, second, third, core, rel) in enumerate(keyed):
        place[rel] = row
        chunks.setdefault((group, first, second), []).append((row, third, core))
    return place, chunks, [k[-1] for k in keyed]


PLACE, CHUNKS, STEPS = make_plan()


def my_index():
    at = [lax.axis_index(a) for a in AXES]
    return ((at[0] * 4 + at[1]) * 2 + at[2]) * 4 + at[3]


def partner(**steps):
    return tuple(
        jnp.bitwise_xor(lax.axis_index(a), steps[a]) if steps.get(a) else lax.axis_index(a)
        for a in AXES
    )


def along(axis, step, core=0):
    return partner(**{axis: step, "c": core})


def place_kernel(slot_ref, total_ref, pages_ref, out_ref, load_ref, place_ref, sem):
    me = my_index()
    for rel in range(DEVICES):
        place_ref[rel] = int(PLACE[rel])

    @pl.loop(0, DEVICES)
    def _(e):
        row = place_ref[jnp.bitwise_xor(e, me)]
        pltpu.make_async_copy(pages_ref.at[row], out_ref.at[slot_ref[0, e], 0], sem).start()

    load_ref[...] = total_ref[...] * (1.0 / 2048.0)
    pltpu.make_async_copy(pages_ref, pages_ref, sem).wait()


def exchange_kernel(
    rate_in, table_in, slots_in, stored_ref,
    pages_ref, slot_out_ref, load_ref,
    rate_ref, table_ref, slots_ref, stay, send_ref, mid1, mid2, index_row, index, known, row1, row2, row3, part1, part2, part3,
    sent, got1, got2, got3, local, small_sent, small_got,
):
    x, z, c, y = (lax.axis_index(a) for a in AXES)
    me = my_index()
    row = c * 4 + y
    remote = lambda src, dst, ss, rs, dev: pltpu.make_async_remote_copy(
        src, dst, ss, rs, device_id=dev, device_id_type=pl.DeviceIdType.MESH
    )

    def wait(ref, sem):
        pltpu.make_async_copy(ref, ref, sem).wait()

    small = [
        pltpu.make_async_copy(src, dst, local.at[4 + k])
        for k, (src, dst) in enumerate(
            ((slots_in, slots_ref), (table_in, table_ref), (rate_in, rate_ref))
        )
    ]
    load = pltpu.make_async_copy(stored_ref.at[:, 0], stay, local.at[2])
    keep = pltpu.make_async_copy(slots_in, known.at[x, z, pl.ds(row, 1)], local.at[0])
    small[0].start()
    load.start()
    barrier = pltpu.get_barrier_semaphore()
    peers = [partner(c=1)] + [along(a, s, k) for a in "xyz" for s in AWAY for k in (0, 1)]
    for dev in peers:
        pl.semaphore_signal(barrier, inc=1, device_id=dev, device_id_type=pl.DeviceIdType.MESH)
    keep.start()
    small[1].start()
    small[2].start()
    small[0].wait()
    down = lax.broadcasted_iota(jnp.int32, (DEVICES, DEVICES), 0)
    right = lax.broadcasted_iota(jnp.int32, (DEVICES, DEVICES), 1)
    step_row = jnp.bitwise_xor(lax.shift_right_logical(slots_ref[...], 7), me)
    found = jnp.where(down == step_row, right, 0).astype(jnp.float32)
    index_row[...] = jnp.bitwise_and(
        jnp.sum(found.T, axis=0, keepdims=True).astype(jnp.int32), DEVICES - 1
    )
    pl.semaphore_wait(barrier, len(peers))
    fetch = pltpu.make_async_copy(index_row, index, local.at[3])
    fetch.start()
    fetch.wait()
    load.wait()

    cell = [partner(c=k, y=s) for k in (0, 1) for s in range(4) if k or s]

    def span(key):
        rows = CHUNKS[key]
        return pl.ds(rows[0][0], len(rows))

    def spot(key):
        return (key[0] * 4 + key[1]) * 4 + key[2]

    def source(key):
        return mid2 if key[2] else (mid1 if key[1] else send_ref)

    def phase1(key):
        remote(
            send_ref.at[span(key)], mid1.at[span(key)], sent.at[0], got1.at[spot(key)],
            along(ORDERS[key[0]][0], key[1]),
        ).start()

    def phase2(key):
        src = mid1 if key[1] else send_ref
        remote(
            src.at[span(key)], mid2.at[span(key)], sent.at[1], got2.at[spot(key)],
            along(ORDERS[key[0]][1], key[2]),
        ).start()

    def phase3(key):
        src = source(key)
        for page, step, core in CHUNKS[key]:
            if step or core:
                remote(
                    src.at[page], pages_ref.at[page], sent.at[2], got3,
                    along(ORDERS[key[0]][2], step, core),
                ).start()
            else:
                pltpu.make_async_copy(src.at[page], pages_ref.at[page], local.at[1]).start()

    def start1(second):
        for first in AWAY:
            for g in range(3):
                phase1((g, first, second))

    def forward2(second):
        for first in AWAY:
            for g in range(3):
                key = (g, first, second)
                wait(mid1.at[span(key)], got1.at[spot(key)])
                phase2(key)

    def pack(keys):
        for key in keys:
            for page, _, _ in CHUNKS[key]:
                send_ref[page] = stay[index[0, STEPS[page]]]

    def block(second):
        return [(g, first, second) for first in AWAY for g in range(3)]

    def near(seconds):
        return [(g, 0, second) for second in seconds for g in range(3)]

    def tell(src, dst, k, devs):
        for dev in devs:
            remote(src, dst, small_sent.at[k], small_got.at[k], dev).start()

    zs = [partner(z=s) for s in AWAY]
    xs = [partner(x=s) for s in AWAY]

    pack(block(2))
    tell(slots_ref, known.at[x, z, pl.ds(row, 1)], 0, cell)
    pack(block(1)[:3])
    start1(2)
    pack(block(1)[3:])
    pack(block(3))
    start1(1)
    pack(block(0))
    keep.wait()
    wait(known.at[0, 0, pl.ds(0, 7)], small_got.at[0])
    tell(known.at[x, z], known.at[x, z], 1, zs)
    start1(3)
    wait(known.at[0, pl.ds(0, 3)], small_got.at[1])
    tell(known.at[x], known.at[x], 2, xs)
    pack(near(AWAY))
    start1(0)
    pack(near((0,)))
    for second in AWAY:
        for g in range(3):
            phase2((g, 0, second))
    wait(known.at[pl.ds(0, 3)], small_got.at[2])

    small[1].wait()
    small[2].wait()
    slots = known[...].reshape(DEVICES, DEVICES)
    owner = lax.shift_right_logical(slots, 7)
    owner_t = owner.astype(jnp.float32).T.astype(jnp.bfloat16)

    def entry(r, acc):
        page = table_ref[pl.ds(r, 1), :]
        high = lax.shift_right_logical(page, 7)
        low = jnp.bitwise_and(page, 127)
        pick = jnp.where(down == high, 1.0, 0.0).astype(jnp.bfloat16)
        column = jnp.dot(owner_t, pick, preferred_element_type=jnp.float32)
        mine = jnp.sum(jnp.where(down == low, column, 0.0), axis=0, keepdims=True)
        return acc + jnp.where(down == mine.astype(jnp.int32), rate_ref[r], 0.0)

    acc = lax.fori_loop(0, 16, entry, jnp.zeros((DEVICES, DEVICES), jnp.float32))
    first_sum = jnp.sum(acc.T, axis=0, keepdims=True)
    part1[...] = first_sum
    row1[pl.ds(row, 1), :] = first_sum
    to_me = jnp.where(owner == me, jnp.bitwise_and(slots, 127), 0).astype(jnp.float32)
    slot_out_ref[...] = jnp.sum(to_me.T, axis=0, keepdims=True).astype(jnp.int32)

    tell(part1, row1.at[pl.ds(row, 1)], 3, cell)
    for second in AWAY:
        forward2(second)
    wait(row1.at[pl.ds(0, 7)], small_got.at[3])
    second_sum = jnp.sum(row1[...], axis=0, keepdims=True)
    part2[...] = second_sum
    row2[pl.ds(z, 1), :] = second_sum
    for g in range(3):
        phase3((g, 0, 0))
    tell(part2, row2.at[pl.ds(z, 1)], 4, zs)
    for first in AWAY:
        for g in range(3):
            key = (g, first, 0)
            wait(mid1.at[span(key)], got1.at[spot(key)])
            phase3(key)
    for second in AWAY:
        for g in range(3):
            key = (g, 0, second)
            wait(mid2.at[span(key)], got2.at[spot(key)])
            phase3(key)
    for second in AWAY:
        if second == LATE_SUM:
            wait(row2.at[pl.ds(0, 3)], small_got.at[4])
            third_sum = jnp.sum(row2[...], axis=0, keepdims=True)
            part3[...] = third_sum
            row3[pl.ds(x, 1), :] = third_sum
        for first in AWAY:
            for g in range(3):
                key = (g, first, second)
                wait(mid2.at[span(key)], got2.at[spot(key)])
                phase3(key)
            if second == LATE_SUM and first == 2:
                tell(part3, row3.at[pl.ds(x, 1)], 5, xs)
    wait(row3.at[pl.ds(0, 3)], small_got.at[5])
    load_ref[...] = jnp.sum(row3[...], axis=0, keepdims=True)

    pages = [sum(len(v) for k, v in CHUNKS.items() if k[i]) for i in (1, 2)]
    far = sum(1 for v in CHUNKS.values() for _, s, k in v if s or k)
    wait(send_ref.at[pl.ds(0, pages[0])], sent.at[0])
    wait(send_ref.at[pl.ds(0, pages[1])], sent.at[1])
    wait(send_ref.at[pl.ds(0, far)], sent.at[2])
    wait(pages_ref.at[pl.ds(0, far)], got3)
    wait(pages_ref.at[pl.ds(0, DEVICES - far)], local.at[1])
    wait(known.at[0, 0, pl.ds(0, 7)], small_sent.at[0])
    wait(known.at[0, pl.ds(0, 3)], small_sent.at[1])
    wait(known.at[pl.ds(0, 3)], small_sent.at[2])
    wait(row1.at[pl.ds(0, 7)], small_sent.at[3])
    wait(row2.at[pl.ds(0, 3)], small_sent.at[4])
    wait(row3.at[pl.ds(0, 3)], small_sent.at[5])


SMEM = pl.BlockSpec(memory_space=pltpu.SMEM)
VMEM = pl.BlockSpec(memory_space=pltpu.VMEM)
HBM = pl.BlockSpec(memory_space=pltpu.HBM)


def on_device(kv_pages, new_slot, request_rate, page_table):
    block = jax.ShapeDtypeStruct((DEVICES,) + kv_pages.shape[2:], kv_pages.dtype)
    buffer = pltpu.VMEM(block.shape, block.dtype)
    line = lambda dtype: jax.ShapeDtypeStruct((1, DEVICES), dtype)
    row = lambda n, dtype=jnp.float32: pltpu.VMEM((n, DEVICES), dtype)
    dma = pltpu.SemaphoreType.DMA
    arrived, slot, total = pl.pallas_call(
        exchange_kernel,
        out_shape=(block, line(jnp.int32), line(jnp.float32)),
        in_specs=[HBM] * 4,
        out_specs=(VMEM, VMEM, VMEM),
        scratch_shapes=[
            pltpu.SMEM((16,), jnp.float32), row(16, jnp.int32), row(1, jnp.int32),
            buffer, buffer, buffer, buffer, row(1, jnp.int32), pltpu.SMEM((1, DEVICES), jnp.int32),
            pltpu.VMEM((4, 4, 8, DEVICES), jnp.int32),
            row(8), row(4), row(4), row(1), row(1), row(1),
            dma((3,)), dma((48,)), dma((48,)), dma, dma((7,)), dma((6,)), dma((6,)),
        ],
        compiler_params=pltpu.CompilerParams(
            collective_id=0, has_side_effects=True, vmem_limit_bytes=36 << 20
        ),
        name="exchange",
    )(*(pltpu.with_memory_space_constraint(v, pltpu.HBM)
        for v in (request_rate, page_table, new_slot.reshape(1, DEVICES), kv_pages)))
    migrated, load = pl.pallas_call(
        place_kernel,
        out_shape=(jax.ShapeDtypeStruct(kv_pages.shape, kv_pages.dtype), line(jnp.float32)),
        in_specs=[SMEM, VMEM, VMEM],
        out_specs=(HBM, VMEM),
        scratch_shapes=[pltpu.SMEM((DEVICES,), jnp.int32), dma],
        compiler_params=pltpu.CompilerParams(vmem_limit_bytes=12 << 20),
        name="place",
    )(slot, total, arrived)
    return migrated, load.reshape(DEVICES)


def solution(mesh):
    split = Mesh(mesh.devices.reshape(4, 4, 2, mesh.shape["dev"]), AXES)
    placed = (P(AXES, None, None, None, None), P(AXES), P(AXES), P(AXES, None))
    return jax.shard_map(
        on_device,
        mesh=split,
        in_specs=placed,
        out_specs=(P(AXES, None, None, None, None), P()),
        check_vma=False,
    )
```

```python
import jax
import jax.numpy as jnp
import numpy as np
from jax import lax
from jax.experimental import pallas as pl
from jax.experimental.pallas import tpu as pltpu
from jax.sharding import Mesh
from jax.sharding import PartitionSpec as P

AXES = ("x", "z", "c", "y")
SIZE = {"x": 4, "z": 4, "c": 2, "y": 4}
DEVICES = 128
ORDERS = (("x", "y", "z"), ("y", "z", "x"), ("z", "x", "y"))
LATE = (2, 1, 3, 0)
AWAY = (2, 1, 3)
LATE_SUM = 3


def make_plan():
    keyed = []
    for rel in range(DEVICES):
        step = {"x": rel // 32, "z": rel // 8 % 4, "c": rel // 4 % 2, "y": rel % 4}
        group = sum(step.values()) % 3
        first, second, third = (step[a] for a in ORDERS[group])
        keyed.append((group, first, second, third, step["c"], rel))
    keyed.sort()
    place = np.zeros((DEVICES,), np.int32)
    chunks = {}
    for row, (group, first, second, third, core, rel) in enumerate(keyed):
        place[rel] = row
        chunks.setdefault((group, first, second), []).append((row, third, core))
    return place, chunks, [k[-1] for k in keyed]


PLACE, CHUNKS, STEPS = make_plan()


def my_index():
    at = [lax.axis_index(a) for a in AXES]
    return ((at[0] * 4 + at[1]) * 2 + at[2]) * 4 + at[3]


def core_first(index):
    return (
        (index & 4) * 16 + (lax.shift_right_logical(index, 5)) * 16
        + (lax.shift_right_logical(index, 1) & 12) + (index & 3)
    )


def partner(**steps):
    return tuple(
        jnp.bitwise_xor(lax.axis_index(a), steps[a]) if steps.get(a) else lax.axis_index(a)
        for a in AXES
    )


def along(axis, step, core=0):
    return partner(**{axis: step, "c": core})


def place_kernel(slot_ref, total_ref, pages_ref, out_ref, load_ref, place_ref, sem):
    me = core_first(my_index())
    for rel in range(DEVICES):
        at = (rel & 4) * 16 + (rel >> 5) * 16 + (rel >> 1 & 12) + (rel & 3)
        place_ref[at] = int(PLACE[rel])

    @pl.loop(0, DEVICES)
    def _(e):
        row = place_ref[jnp.bitwise_xor(e, me)]
        pltpu.make_async_copy(pages_ref.at[row], out_ref.at[slot_ref[0, e], 0], sem).start()

    load_ref[...] = total_ref[...] * (1.0 / 2048.0)
    pltpu.make_async_copy(pages_ref, pages_ref, sem).wait()


def exchange_kernel(
    rate_in, table_in, slots_in, stored_ref,
    pages_ref, slot_out_ref, load_ref,
    rate_ref, table_ref, slots_ref, stay, send_ref, mid1, mid2, index_row, index, known, row0, row1, row2, row3, part0, part1, part2, part3,
    sent, got1, got2, got3, local, small_sent, small_got,
):
    x, z, c, y = (lax.axis_index(a) for a in AXES)
    me = my_index()
    row = z * 4 + y
    remote = lambda src, dst, ss, rs, dev: pltpu.make_async_remote_copy(
        src, dst, ss, rs, device_id=dev, device_id_type=pl.DeviceIdType.MESH
    )

    def wait(ref, sem):
        pltpu.make_async_copy(ref, ref, sem).wait()

    small = [
        pltpu.make_async_copy(src, dst, local.at[4 + k])
        for k, (src, dst) in enumerate(
            ((slots_in, slots_ref), (table_in, table_ref), (rate_in, rate_ref))
        )
    ]
    load = pltpu.make_async_copy(stored_ref.at[:, 0], stay, local.at[2])
    keep = pltpu.make_async_copy(slots_in, known.at[c, x, pl.ds(row, 1)], local.at[0])
    small[0].start()
    load.start()
    barrier = pltpu.get_barrier_semaphore()
    peers = [partner(c=1)] + [along(a, s, k) for a in "xyz" for s in AWAY for k in (0, 1)]
    for dev in peers:
        pl.semaphore_signal(barrier, inc=1, device_id=dev, device_id_type=pl.DeviceIdType.MESH)
    keep.start()
    small[1].start()
    small[2].start()
    small[0].wait()
    down = lax.broadcasted_iota(jnp.int32, (DEVICES, DEVICES), 0)
    right = lax.broadcasted_iota(jnp.int32, (DEVICES, DEVICES), 1)
    step_row = jnp.bitwise_xor(lax.shift_right_logical(slots_ref[...], 7), me)
    found = jnp.where(down == step_row, right, 0).astype(jnp.float32)
    index_row[...] = jnp.bitwise_and(
        jnp.sum(found.T, axis=0, keepdims=True).astype(jnp.int32), DEVICES - 1
    )
    fetch = pltpu.make_async_copy(index_row, index, local.at[3])
    fetch.start()
    fetch.wait()
    load.wait()

    twin = [partner(c=1)]
    ys = [partner(y=s) for s in AWAY]

    def span(key):
        rows = CHUNKS[key]
        return pl.ds(rows[0][0], len(rows))

    def spot(key):
        return (key[0] * 4 + key[1]) * 4 + key[2]

    def source(key):
        return mid2 if key[2] else (mid1 if key[1] else send_ref)

    def phase1(key):
        remote(
            send_ref.at[span(key)], mid1.at[span(key)], sent.at[0], got1.at[spot(key)],
            along(ORDERS[key[0]][0], key[1]),
        ).start()

    def phase2(key):
        src = mid1 if key[1] else send_ref
        remote(
            src.at[span(key)], mid2.at[span(key)], sent.at[1], got2.at[spot(key)],
            along(ORDERS[key[0]][1], key[2]),
        ).start()

    def phase3(key):
        src = source(key)
        for page, step, core in sorted(CHUNKS[key], key=lambda v: v[1] != 2):
            if step or core:
                remote(
                    src.at[page], pages_ref.at[page], sent.at[2], got3,
                    along(ORDERS[key[0]][2], step, core),
                ).start()
            else:
                pltpu.make_async_copy(src.at[page], pages_ref.at[page], local.at[1]).start()

    def start1(second):
        for first in AWAY:
            for g in range(3):
                phase1((g, first, second))

    def forward2(second):
        for first in AWAY:
            for g in range(3):
                key = (g, first, second)
                wait(mid1.at[span(key)], got1.at[spot(key)])
                phase2(key)

    def pack(keys):
        for key in keys:
            for page, _, _ in CHUNKS[key]:
                send_ref[page] = stay[index[0, STEPS[page]]]

    def block(second):
        return [(g, first, second) for first in AWAY for g in range(3)]

    def near(seconds):
        return [(g, 0, second) for second in seconds for g in range(3)]

    def tell(src, dst, k, devs):
        for dev in devs:
            remote(src, dst, small_sent.at[k], small_got.at[k], dev).start()

    zs = [partner(z=s) for s in AWAY]
    xs = [partner(x=s) for s in AWAY]

    front = block(2) + block(1)
    pack(front[:6])
    pl.semaphore_wait(barrier, len(peers))
    for at in (0, 3, 6):
        for key in front[at : at + 3]:
            phase1(key)
        pack(front[at + 6 : at + 9])
    tell(slots_ref, known.at[c, x, pl.ds(row, 1)], 0, ys)
    pack(front[15:])
    for key in front[9:]:
        phase1(key)
    pack(block(3))
    pack(block(0))
    keep.wait()
    wait(known.at[0, 0, pl.ds(0, 3)], small_got.at[0])
    tell(known.at[c, x, pl.ds(z * 4, 4)], known.at[c, x, pl.ds(z * 4, 4)], 1, zs)
    start1(3)
    pack(near(AWAY))
    wait(known.at[0, 0, pl.ds(0, 12)], small_got.at[1])
    tell(known.at[c, x], known.at[c, x], 2, xs)
    start1(0)
    pack(near((0,)))
    for second in AWAY:
        for g in range(3):
            phase2((g, 0, second))
    wait(known.at[0, pl.ds(0, 3)], small_got.at[2])
    tell(known.at[c], known.at[c], 6, twin)
    wait(known.at[0], small_got.at[6])

    small[1].wait()
    small[2].wait()
    slots = known[...].reshape(DEVICES, DEVICES)
    owner = lax.shift_right_logical(slots, 7)
    owner_t = owner.astype(jnp.float32).T.astype(jnp.bfloat16)

    def entry(r, acc):
        page = table_ref[pl.ds(r, 1), :]
        high = core_first(lax.shift_right_logical(page, 7))
        low = jnp.bitwise_and(page, 127)
        pick = jnp.where(down == high, 1.0, 0.0).astype(jnp.bfloat16)
        column = jnp.dot(owner_t, pick, preferred_element_type=jnp.float32)
        mine = jnp.sum(jnp.where(down == low, column, 0.0), axis=0, keepdims=True)
        return acc + jnp.where(down == mine.astype(jnp.int32), rate_ref[r], 0.0)

    acc = lax.fori_loop(0, 16, entry, jnp.zeros((DEVICES, DEVICES), jnp.float32))
    first_sum = jnp.sum(acc.T, axis=0, keepdims=True)
    part0[...] = first_sum
    to_me = jnp.where(owner == me, jnp.bitwise_and(slots, 127), 0).astype(jnp.float32)
    slot_out_ref[...] = jnp.sum(to_me.T, axis=0, keepdims=True).astype(jnp.int32)

    tell(part0, row0, 7, twin)
    wait(row0, small_got.at[7])
    first_sum = part0[...] + row0[...]
    part1[...] = first_sum
    row1[pl.ds(y, 1), :] = first_sum
    forward2(AWAY[0])
    tell(part1, row1.at[pl.ds(y, 1)], 3, ys)
    for second in AWAY[1:]:
        forward2(second)
    wait(row1.at[pl.ds(0, 3)], small_got.at[3])
    second_sum = jnp.sum(row1[...], axis=0, keepdims=True)
    part2[...] = second_sum
    row2[pl.ds(z, 1), :] = second_sum
    for g in range(3):
        phase3((g, 0, 0))
    tell(part2, row2.at[pl.ds(z, 1)], 4, zs)
    for first in AWAY:
        for g in range(3):
            key = (g, first, 0)
            wait(mid1.at[span(key)], got1.at[spot(key)])
            phase3(key)
    for second in AWAY:
        for g in range(3):
            key = (g, 0, second)
            wait(mid2.at[span(key)], got2.at[spot(key)])
            phase3(key)
    for second in AWAY:
        if second == LATE_SUM:
            wait(row2.at[pl.ds(0, 3)], small_got.at[4])
            third_sum = jnp.sum(row2[...], axis=0, keepdims=True)
            part3[...] = third_sum
            row3[pl.ds(x, 1), :] = third_sum
        for first in AWAY:
            for g in range(3):
                key = (g, first, second)
                wait(mid2.at[span(key)], got2.at[spot(key)])
                phase3(key)
            if second == LATE_SUM and first == 2:
                tell(part3, row3.at[pl.ds(x, 1)], 5, xs)
    wait(row3.at[pl.ds(0, 3)], small_got.at[5])
    load_ref[...] = jnp.sum(row3[...], axis=0, keepdims=True)

    pages = [sum(len(v) for k, v in CHUNKS.items() if k[i]) for i in (1, 2)]
    far = sum(1 for v in CHUNKS.values() for _, s, k in v if s or k)
    wait(send_ref.at[pl.ds(0, pages[0])], sent.at[0])
    wait(send_ref.at[pl.ds(0, pages[1])], sent.at[1])
    wait(send_ref.at[pl.ds(0, far)], sent.at[2])
    wait(pages_ref.at[pl.ds(0, far)], got3)
    wait(pages_ref.at[pl.ds(0, DEVICES - far)], local.at[1])
    wait(known.at[0, 0, pl.ds(0, 3)], small_sent.at[0])
    wait(known.at[0, 0, pl.ds(0, 12)], small_sent.at[1])
    wait(known.at[0, pl.ds(0, 3)], small_sent.at[2])
    wait(known.at[0], small_sent.at[6])
    wait(row0, small_sent.at[7])
    wait(row1.at[pl.ds(0, 3)], small_sent.at[3])
    wait(row2.at[pl.ds(0, 3)], small_sent.at[4])
    wait(row3.at[pl.ds(0, 3)], small_sent.at[5])


SMEM = pl.BlockSpec(memory_space=pltpu.SMEM)
VMEM = pl.BlockSpec(memory_space=pltpu.VMEM)
HBM = pl.BlockSpec(memory_space=pltpu.HBM)


def on_device(kv_pages, new_slot, request_rate, page_table):
    block = jax.ShapeDtypeStruct((DEVICES,) + kv_pages.shape[2:], kv_pages.dtype)
    buffer = pltpu.VMEM(block.shape, block.dtype)
    line = lambda dtype: jax.ShapeDtypeStruct((1, DEVICES), dtype)
    row = lambda n, dtype=jnp.float32: pltpu.VMEM((n, DEVICES), dtype)
    dma = pltpu.SemaphoreType.DMA
    arrived, slot, total = pl.pallas_call(
        exchange_kernel,
        out_shape=(block, line(jnp.int32), line(jnp.float32)),
        in_specs=[HBM] * 4,
        out_specs=(VMEM, VMEM, VMEM),
        scratch_shapes=[
            pltpu.SMEM((16,), jnp.float32), row(16, jnp.int32), row(1, jnp.int32),
            buffer, buffer, buffer, buffer, row(1, jnp.int32), pltpu.SMEM((1, DEVICES), jnp.int32),
            pltpu.VMEM((2, 4, 16, DEVICES), jnp.int32),
            row(1), row(4), row(4), row(4), row(1), row(1), row(1), row(1),
            dma((3,)), dma((48,)), dma((48,)), dma, dma((7,)), dma((8,)), dma((8,)),
        ],
        compiler_params=pltpu.CompilerParams(
            collective_id=0, has_side_effects=True, vmem_limit_bytes=36 << 20
        ),
        name="exchange",
    )(*(pltpu.with_memory_space_constraint(v, pltpu.HBM)
        for v in (request_rate, page_table, new_slot.reshape(1, DEVICES), kv_pages)))
    migrated, load = pl.pallas_call(
        place_kernel,
        out_shape=(jax.ShapeDtypeStruct(kv_pages.shape, kv_pages.dtype), line(jnp.float32)),
        in_specs=[SMEM, VMEM, VMEM],
        out_specs=(HBM, VMEM),
        scratch_shapes=[pltpu.SMEM((DEVICES,), jnp.int32), dma],
        compiler_params=pltpu.CompilerParams(vmem_limit_bytes=12 << 20),
        name="place",
    )(slot, total, arrived)
    return migrated, load.reshape(DEVICES)


def solution(mesh):
    split = Mesh(mesh.devices.reshape(4, 4, 2, mesh.shape["dev"]), AXES)
    placed = (P(AXES, None, None, None, None), P(AXES), P(AXES), P(AXES, None))
    return jax.shard_map(
        on_device,
        mesh=split,
        in_specs=placed,
        out_specs=(P(AXES, None, None, None, None), P()),
        check_vma=False,
    )
```

```python
import jax
import jax.numpy as jnp
import numpy as np
from jax import lax
from jax.experimental import pallas as pl
from jax.experimental.pallas import tpu as pltpu
from jax.sharding import Mesh
from jax.sharding import PartitionSpec as P

AXES = ("x", "z", "c", "y")
SIZE = {"x": 4, "z": 4, "c": 2, "y": 4}
DEVICES = 128
ORDERS = (("x", "y", "z"), ("y", "z", "x"), ("z", "x", "y"))
LATE = (2, 1, 3, 0)
AWAY = (2, 1, 3)
LATE_SUM = 3


def make_plan():
    keyed = []
    for rel in range(DEVICES):
        step = {"x": rel // 32, "z": rel // 8 % 4, "c": rel // 4 % 2, "y": rel % 4}
        group = sum(step.values()) % 3
        first, second, third = (step[a] for a in ORDERS[group])
        keyed.append((group, first, second, third, step["c"], rel))
    keyed.sort()
    place = np.zeros((DEVICES,), np.int32)
    chunks = {}
    for row, (group, first, second, third, core, rel) in enumerate(keyed):
        place[rel] = row
        chunks.setdefault((group, first, second), []).append((row, third, core))
    return place, chunks, [k[-1] for k in keyed]


PLACE, CHUNKS, STEPS = make_plan()


def my_index():
    at = [lax.axis_index(a) for a in AXES]
    return ((at[0] * 4 + at[1]) * 2 + at[2]) * 4 + at[3]


def core_first(index):
    return (
        (index & 4) * 16 + (lax.shift_right_logical(index, 5)) * 16
        + (lax.shift_right_logical(index, 1) & 12) + (index & 3)
    )


def partner(**steps):
    return tuple(
        jnp.bitwise_xor(lax.axis_index(a), steps[a]) if steps.get(a) else lax.axis_index(a)
        for a in AXES
    )


def along(axis, step, core=0):
    return partner(**{axis: step, "c": core})


def place_kernel(slot_in, total_ref, pages_ref, out_ref, load_ref, slot_ref, place_ref, sems):
    fetch = pltpu.make_async_copy(slot_in, slot_ref, sems.at[0])
    fetch.start()
    load = pltpu.make_async_copy(total_ref, load_ref, sems.at[1])
    load.start()
    me = core_first(my_index())
    for rel in range(DEVICES):
        at = (rel & 4) * 16 + (rel >> 5) * 16 + (rel >> 1 & 12) + (rel & 3)
        place_ref[at] = int(PLACE[rel])
    fetch.wait()

    @pl.loop(0, DEVICES)
    def _(e):
        row = place_ref[jnp.bitwise_xor(e, me)]
        pltpu.make_async_copy(pages_ref.at[row], out_ref.at[slot_ref[0, e], 0], sems.at[2]).start()

    load.wait()
    pltpu.make_async_copy(pages_ref, pages_ref, sems.at[2]).wait()


def exchange_kernel(
    rate_in, table_in, slots_in, stored_ref,
    pages_ref, slot_out_ref, load_ref,
    rate_ref, table_ref, slots_ref, stay, send_ref, mid1, mid2, index_row, index, known, row0, row1, row2, row3, part0, part1, part2, part3,
    sent, got1, got2, got3, local, small_sent, small_got,
):
    x, z, c, y = (lax.axis_index(a) for a in AXES)
    me = my_index()
    row = z * 4 + y
    remote = lambda src, dst, ss, rs, dev: pltpu.make_async_remote_copy(
        src, dst, ss, rs, device_id=dev, device_id_type=pl.DeviceIdType.MESH
    )

    def wait(ref, sem):
        pltpu.make_async_copy(ref, ref, sem).wait()

    small = [
        pltpu.make_async_copy(src, dst, local.at[4 + k])
        for k, (src, dst) in enumerate(
            ((slots_in, slots_ref), (table_in, table_ref), (rate_in, rate_ref))
        )
    ]
    load = pltpu.make_async_copy(stored_ref.at[:, 0], stay, local.at[2])
    keep = pltpu.make_async_copy(slots_in, known.at[c, x, pl.ds(row, 1)], local.at[0])
    small[0].start()
    load.start()
    barrier = pltpu.get_barrier_semaphore()
    peers = [partner(c=1)] + [along(a, s, k) for a in "xyz" for s in AWAY for k in (0, 1)]
    for dev in peers:
        pl.semaphore_signal(barrier, inc=1, device_id=dev, device_id_type=pl.DeviceIdType.MESH)
    keep.start()
    small[1].start()
    small[2].start()
    small[0].wait()
    down = lax.broadcasted_iota(jnp.int32, (DEVICES, DEVICES), 0)
    right = lax.broadcasted_iota(jnp.int32, (DEVICES, DEVICES), 1)
    step_row = jnp.bitwise_xor(lax.shift_right_logical(slots_ref[...], 7), me)
    found = jnp.where(down == step_row, right, 0).astype(jnp.float32)
    index_row[...] = jnp.bitwise_and(
        jnp.sum(found.T, axis=0, keepdims=True).astype(jnp.int32), DEVICES - 1
    )
    fetch = pltpu.make_async_copy(index_row, index, local.at[3])
    fetch.start()
    fetch.wait()
    load.wait()

    twin = [partner(c=1)]
    ys = [partner(y=s) for s in AWAY]

    def span(key):
        rows = CHUNKS[key]
        return pl.ds(rows[0][0], len(rows))

    def spot(key):
        return (key[0] * 4 + key[1]) * 4 + key[2]

    def source(key):
        return mid2 if key[2] else (mid1 if key[1] else send_ref)

    def phase1(key):
        remote(
            send_ref.at[span(key)], mid1.at[span(key)], sent.at[0], got1.at[spot(key)],
            along(ORDERS[key[0]][0], key[1]),
        ).start()

    def phase2(key):
        src = mid1 if key[1] else send_ref
        remote(
            src.at[span(key)], mid2.at[span(key)], sent.at[1], got2.at[spot(key)],
            along(ORDERS[key[0]][1], key[2]),
        ).start()

    def phase3(key):
        src = source(key)
        for page, step, core in sorted(CHUNKS[key], key=lambda v: v[1] != 2):
            if step or core:
                remote(
                    src.at[page], pages_ref.at[page], sent.at[2], got3,
                    along(ORDERS[key[0]][2], step, core),
                ).start()
            else:
                pltpu.make_async_copy(src.at[page], pages_ref.at[page], local.at[1]).start()

    def start1(second):
        for first in AWAY:
            for g in range(3):
                phase1((g, first, second))

    def forward2(second):
        for first in AWAY:
            for g in range(3):
                key = (g, first, second)
                wait(mid1.at[span(key)], got1.at[spot(key)])
                phase2(key)

    def pack(keys):
        for key in keys:
            for page, _, _ in CHUNKS[key]:
                send_ref[page] = stay[index[0, STEPS[page]]]

    def block(second):
        return [(g, first, second) for first in AWAY for g in range(3)]

    def near(seconds):
        return [(g, 0, second) for second in seconds for g in range(3)]

    def tell(src, dst, k, devs):
        for dev in devs:
            remote(src, dst, small_sent.at[k], small_got.at[k], dev).start()

    zs = [partner(z=s) for s in AWAY]
    xs = [partner(x=s) for s in AWAY]

    front = block(2) + block(1)
    pack(front[:6])
    pl.semaphore_wait(barrier, len(peers))
    for at in (0, 3, 6):
        for key in front[at : at + 3]:
            phase1(key)
        if at == 0:
            tell(slots_ref, known.at[c, x, pl.ds(row, 1)], 0, ys)
        pack(front[at + 6 : at + 9])
    keep.wait()
    wait(known.at[0, 0, pl.ds(0, 3)], small_got.at[0])
    tell(known.at[c, x, pl.ds(z * 4, 4)], known.at[c, x, pl.ds(z * 4, 4)], 1, zs)
    pack(front[15:])
    for key in front[9:]:
        phase1(key)
    pack(block(3))
    pack(block(0))
    wait(known.at[0, 0, pl.ds(0, 12)], small_got.at[1])
    tell(known.at[c, x], known.at[c, x], 2, xs)
    start1(3)
    pack(near(AWAY))
    start1(0)
    pack(near((0,)))
    for second in AWAY:
        for g in range(3):
            phase2((g, 0, second))
    wait(known.at[0, pl.ds(0, 3)], small_got.at[2])
    tell(known.at[c], known.at[c], 6, twin)
    wait(known.at[0], small_got.at[6])

    small[1].wait()
    small[2].wait()
    slots = known[...].reshape(DEVICES, DEVICES)
    owner = lax.shift_right_logical(slots, 7)
    owner_t = owner.astype(jnp.float32).T.astype(jnp.bfloat16)

    def entry(r, acc):
        page = table_ref[pl.ds(r, 1), :]
        high = core_first(lax.shift_right_logical(page, 7))
        low = jnp.bitwise_and(page, 127)
        pick = jnp.where(down == high, 1.0, 0.0).astype(jnp.bfloat16)
        column = jnp.dot(owner_t, pick, preferred_element_type=jnp.float32)
        mine = jnp.sum(jnp.where(down == low, column, 0.0), axis=0, keepdims=True)
        return acc + jnp.where(down == mine.astype(jnp.int32), rate_ref[r], 0.0)

    acc = lax.fori_loop(0, 16, entry, jnp.zeros((DEVICES, DEVICES), jnp.float32))
    first_sum = jnp.sum(acc.T, axis=0, keepdims=True)
    part0[...] = first_sum
    to_me = jnp.where(owner == me, jnp.bitwise_and(slots, 127), 0).astype(jnp.float32)
    slot_out_ref[...] = jnp.sum(to_me.T, axis=0, keepdims=True).astype(jnp.int32)

    tell(part0, row0, 7, twin)
    wait(row0, small_got.at[7])
    first_sum = part0[...] + row0[...]
    part1[...] = first_sum
    row1[pl.ds(y, 1), :] = first_sum
    forward2(AWAY[0])
    tell(part1, row1.at[pl.ds(y, 1)], 3, ys)
    for second in AWAY[1:]:
        forward2(second)
    wait(row1.at[pl.ds(0, 3)], small_got.at[3])
    second_sum = jnp.sum(row1[...], axis=0, keepdims=True)
    part2[...] = second_sum
    row2[pl.ds(z, 1), :] = second_sum
    for g in range(3):
        phase3((g, 0, 0))
    tell(part2, row2.at[pl.ds(z, 1)], 4, zs)
    for first in AWAY:
        for g in range(3):
            key = (g, first, 0)
            wait(mid1.at[span(key)], got1.at[spot(key)])
            phase3(key)
    for second in AWAY:
        for g in range(3):
            key = (g, 0, second)
            wait(mid2.at[span(key)], got2.at[spot(key)])
            phase3(key)
    for second in AWAY:
        if second == LATE_SUM:
            wait(row2.at[pl.ds(0, 3)], small_got.at[4])
            third_sum = jnp.sum(row2[...], axis=0, keepdims=True)
            part3[...] = third_sum
            row3[pl.ds(x, 1), :] = third_sum
        for first in AWAY:
            for g in range(3):
                key = (g, first, second)
                wait(mid2.at[span(key)], got2.at[spot(key)])
                phase3(key)
            if second == LATE_SUM and first == 2:
                tell(part3, row3.at[pl.ds(x, 1)], 5, xs)
    wait(row3.at[pl.ds(0, 3)], small_got.at[5])
    load_ref[...] = jnp.sum(row3[...], axis=0, keepdims=True) * (1.0 / 2048.0)

    pages = [sum(len(v) for k, v in CHUNKS.items() if k[i]) for i in (1, 2)]
    far = sum(1 for v in CHUNKS.values() for _, s, k in v if s or k)
    wait(send_ref.at[pl.ds(0, pages[0])], sent.at[0])
    wait(send_ref.at[pl.ds(0, pages[1])], sent.at[1])
    wait(send_ref.at[pl.ds(0, far)], sent.at[2])
    wait(pages_ref.at[pl.ds(0, far)], got3)
    wait(pages_ref.at[pl.ds(0, DEVICES - far)], local.at[1])
    wait(known.at[0, 0, pl.ds(0, 3)], small_sent.at[0])
    wait(known.at[0, 0, pl.ds(0, 12)], small_sent.at[1])
    wait(known.at[0, pl.ds(0, 3)], small_sent.at[2])
    wait(known.at[0], small_sent.at[6])
    wait(row0, small_sent.at[7])
    wait(row1.at[pl.ds(0, 3)], small_sent.at[3])
    wait(row2.at[pl.ds(0, 3)], small_sent.at[4])
    wait(row3.at[pl.ds(0, 3)], small_sent.at[5])


SMEM = pl.BlockSpec(memory_space=pltpu.SMEM)
VMEM = pl.BlockSpec(memory_space=pltpu.VMEM)
HBM = pl.BlockSpec(memory_space=pltpu.HBM)


def on_device(kv_pages, new_slot, request_rate, page_table):
    block = jax.ShapeDtypeStruct((DEVICES,) + kv_pages.shape[2:], kv_pages.dtype)
    buffer = pltpu.VMEM(block.shape, block.dtype)
    line = lambda dtype: jax.ShapeDtypeStruct((1, DEVICES), dtype)
    row = lambda n, dtype=jnp.float32: pltpu.VMEM((n, DEVICES), dtype)
    dma = pltpu.SemaphoreType.DMA
    arrived, slot, total = pl.pallas_call(
        exchange_kernel,
        out_shape=(block, line(jnp.int32), line(jnp.float32)),
        in_specs=[HBM] * 4,
        out_specs=(VMEM, VMEM, VMEM),
        scratch_shapes=[
            pltpu.SMEM((16,), jnp.float32), row(16, jnp.int32), row(1, jnp.int32),
            buffer, buffer, buffer, buffer, row(1, jnp.int32), pltpu.SMEM((1, DEVICES), jnp.int32),
            pltpu.VMEM((2, 4, 16, DEVICES), jnp.int32),
            row(1), row(4), row(4), row(4), row(1), row(1), row(1), row(1),
            dma((3,)), dma((48,)), dma((48,)), dma, dma((7,)), dma((8,)), dma((8,)),
        ],
        compiler_params=pltpu.CompilerParams(
            collective_id=0, has_side_effects=True, vmem_limit_bytes=36 << 20
        ),
        name="exchange",
    )(*(pltpu.with_memory_space_constraint(v, pltpu.HBM)
        for v in (request_rate, page_table, new_slot.reshape(1, DEVICES), kv_pages)))
    migrated, load = pl.pallas_call(
        place_kernel,
        out_shape=(jax.ShapeDtypeStruct(kv_pages.shape, kv_pages.dtype), line(jnp.float32)),
        in_specs=[VMEM, VMEM, VMEM],
        out_specs=(HBM, HBM),
        scratch_shapes=[
            pltpu.SMEM((1, DEVICES), jnp.int32), pltpu.SMEM((DEVICES,), jnp.int32), dma((3,)),
        ],
        compiler_params=pltpu.CompilerParams(vmem_limit_bytes=12 << 20),
        name="place",
    )(slot, total, arrived)
    return migrated, load.reshape(DEVICES)


def solution(mesh):
    split = Mesh(mesh.devices.reshape(4, 4, 2, mesh.shape["dev"]), AXES)
    placed = (P(AXES, None, None, None, None), P(AXES), P(AXES), P(AXES, None))
    return jax.shard_map(
        on_device,
        mesh=split,
        in_specs=placed,
        out_specs=(P(AXES, None, None, None, None), P()),
        check_vma=False,
    )
```

```python
import jax
import jax.numpy as jnp
import numpy as np
from jax import lax
from jax.experimental import pallas as pl
from jax.experimental.pallas import tpu as pltpu
from jax.sharding import Mesh
from jax.sharding import PartitionSpec as P

AXES = ("x", "z", "c", "y")
SIZE = {"x": 4, "z": 4, "c": 2, "y": 4}
DEVICES = 128
ORDERS = (("x", "y", "z"), ("y", "z", "x"), ("z", "x", "y"))
LATE = (2, 1, 3, 0)
AWAY = (2, 1, 3)
LATE_SUM = 3


def make_plan():
    keyed = []
    for rel in range(DEVICES):
        step = {"x": rel // 32, "z": rel // 8 % 4, "c": rel // 4 % 2, "y": rel % 4}
        group = sum(step.values()) % 3
        first, second, third = (step[a] for a in ORDERS[group])
        keyed.append((group, first, second, third, step["c"], rel))
    keyed.sort()
    place = np.zeros((DEVICES,), np.int32)
    chunks = {}
    for row, (group, first, second, third, core, rel) in enumerate(keyed):
        place[rel] = row
        chunks.setdefault((group, first, second), []).append((row, third, core))
    return place, chunks, [k[-1] for k in keyed]


PLACE, CHUNKS, STEPS = make_plan()


def my_index():
    at = [lax.axis_index(a) for a in AXES]
    return ((at[0] * 4 + at[1]) * 2 + at[2]) * 4 + at[3]


def core_first(index):
    return (
        (index & 4) * 16 + (lax.shift_right_logical(index, 5)) * 16
        + (lax.shift_right_logical(index, 1) & 12) + (index & 3)
    )


def partner(**steps):
    return tuple(
        jnp.bitwise_xor(lax.axis_index(a), steps[a]) if steps.get(a) else lax.axis_index(a)
        for a in AXES
    )


def along(axis, step, core=0):
    return partner(**{axis: step, "c": core})


def place_kernel(slot_in, total_ref, pages_ref, out_ref, load_ref, slot_ref, place_ref, sems):
    fetch = pltpu.make_async_copy(slot_in, slot_ref, sems.at[0])
    fetch.start()
    load = pltpu.make_async_copy(total_ref, load_ref, sems.at[1])
    load.start()
    me = core_first(my_index())
    for rel in range(DEVICES):
        at = (rel & 4) * 16 + (rel >> 5) * 16 + (rel >> 1 & 12) + (rel & 3)
        place_ref[at] = int(PLACE[rel])
    fetch.wait()

    @pl.loop(0, DEVICES)
    def _(e):
        row = place_ref[jnp.bitwise_xor(e, me)]
        pltpu.make_async_copy(pages_ref.at[row], out_ref.at[slot_ref[0, e], 0], sems.at[2]).start()

    load.wait()
    pltpu.make_async_copy(pages_ref, pages_ref, sems.at[2]).wait()


def exchange_kernel(
    rate_in, table_in, slots_in, stored_ref,
    pages_ref, slot_out_ref, load_ref,
    rate_ref, table_ref, slots_ref, stay, send_ref, mid1, mid2, index_row, index, known, row0, row1, row2, row3, part0, part1, part2, part3,
    sent, got1, got2, got3, local, small_sent, small_got,
):
    x, z, c, y = (lax.axis_index(a) for a in AXES)
    me = my_index()
    row = z * 4 + y
    remote = lambda src, dst, ss, rs, dev: pltpu.make_async_remote_copy(
        src, dst, ss, rs, device_id=dev, device_id_type=pl.DeviceIdType.MESH
    )

    def wait(ref, sem):
        pltpu.make_async_copy(ref, ref, sem).wait()

    small = [
        pltpu.make_async_copy(src, dst, local.at[4 + k])
        for k, (src, dst) in enumerate(
            ((slots_in, slots_ref), (table_in, table_ref), (rate_in, rate_ref))
        )
    ]
    load = pltpu.make_async_copy(stored_ref.at[:, 0], stay, local.at[2])
    keep = pltpu.make_async_copy(slots_in, known.at[c, x, pl.ds(row, 1)], local.at[0])
    small[0].start()
    load.start()
    barrier = pltpu.get_barrier_semaphore()
    peers = [partner(c=1)] + [along(a, s) for a in "xyz" for s in AWAY]
    for dev in peers:
        pl.semaphore_signal(barrier, inc=1, device_id=dev, device_id_type=pl.DeviceIdType.MESH)
    keep.start()
    small[1].start()
    small[2].start()
    small[0].wait()
    down = lax.broadcasted_iota(jnp.int32, (DEVICES, DEVICES), 0)
    right = lax.broadcasted_iota(jnp.int32, (DEVICES, DEVICES), 1)
    step_row = jnp.bitwise_xor(lax.shift_right_logical(slots_ref[...], 7), me)
    found = jnp.where(down == step_row, right, 0).astype(jnp.float32)
    index_row[...] = jnp.bitwise_and(
        jnp.sum(found.T, axis=0, keepdims=True).astype(jnp.int32), DEVICES - 1
    )
    fetch = pltpu.make_async_copy(index_row, index, local.at[3])
    fetch.start()
    fetch.wait()
    load.wait()

    twin = [partner(c=1)]
    ys = [partner(y=s) for s in AWAY]

    def span(key):
        rows = CHUNKS[key]
        return pl.ds(rows[0][0], len(rows))

    def spot(key):
        return (key[0] * 4 + key[1]) * 4 + key[2]

    def source(key):
        return mid2 if key[2] else (mid1 if key[1] else send_ref)

    def phase1(key):
        remote(
            send_ref.at[span(key)], mid1.at[span(key)], sent.at[0], got1.at[spot(key)],
            along(ORDERS[key[0]][0], key[1]),
        ).start()

    def phase2(key):
        src = mid1 if key[1] else send_ref
        remote(
            src.at[span(key)], mid2.at[span(key)], sent.at[1], got2.at[spot(key)],
            along(ORDERS[key[0]][1], key[2]),
        ).start()

    def phase3(key):
        src = source(key)
        for page, step, core in sorted(CHUNKS[key], key=lambda v: v[1] != 2):
            if step or core:
                remote(
                    src.at[page], pages_ref.at[page], sent.at[2], got3,
                    along(ORDERS[key[0]][2], step, core),
                ).start()
            else:
                pltpu.make_async_copy(src.at[page], pages_ref.at[page], local.at[1]).start()

    def start1(second):
        for first in AWAY:
            for g in range(3):
                phase1((g, first, second))

    def forward2(second):
        for first in AWAY:
            for g in range(3):
                key = (g, first, second)
                wait(mid1.at[span(key)], got1.at[spot(key)])
                phase2(key)

    def pack(keys):
        for key in keys:
            for page, _, _ in CHUNKS[key]:
                send_ref[page] = stay[index[0, STEPS[page]]]

    def block(second):
        return [(g, first, second) for first in AWAY for g in range(3)]

    def near(seconds):
        return [(g, 0, second) for second in seconds for g in range(3)]

    def tell(src, dst, k, devs):
        for dev in devs:
            remote(src, dst, small_sent.at[k], small_got.at[k], dev).start()

    zs = [partner(z=s) for s in AWAY]
    xs = [partner(x=s) for s in AWAY]

    front = block(2) + block(1)
    pack(front[:6])
    pl.semaphore_wait(barrier, len(peers))
    for at in (0, 3, 6):
        for key in front[at : at + 3]:
            phase1(key)
        if at == 0:
            tell(slots_ref, known.at[c, x, pl.ds(row, 1)], 0, ys)
        pack(front[at + 6 : at + 9])
    keep.wait()
    wait(known.at[0, 0, pl.ds(0, 3)], small_got.at[0])
    tell(known.at[c, x, pl.ds(z * 4, 4)], known.at[c, x, pl.ds(z * 4, 4)], 1, zs)
    pack(front[15:])
    for key in front[9:]:
        phase1(key)
    pack(block(0))
    pack(block(3))
    wait(known.at[0, 0, pl.ds(0, 12)], small_got.at[1])
    tell(known.at[c, x], known.at[c, x], 2, xs)
    start1(0)
    pack(near(AWAY))
    start1(3)
    pack(near((0,)))
    for second in AWAY:
        for g in range(3):
            phase2((g, 0, second))
    wait(known.at[0, pl.ds(0, 3)], small_got.at[2])
    tell(known.at[c], known.at[c], 6, twin)
    wait(known.at[0], small_got.at[6])

    small[1].wait()
    small[2].wait()
    slots = known[...].reshape(DEVICES, DEVICES)
    owner = lax.shift_right_logical(slots, 7)
    owner_t = owner.astype(jnp.float32).T.astype(jnp.bfloat16)

    def entry(r, acc):
        page = table_ref[pl.ds(r, 1), :]
        high = core_first(lax.shift_right_logical(page, 7))
        low = jnp.bitwise_and(page, 127)
        pick = jnp.where(down == high, 1.0, 0.0).astype(jnp.bfloat16)
        column = jnp.dot(owner_t, pick, preferred_element_type=jnp.float32)
        mine = jnp.sum(jnp.where(down == low, column, 0.0), axis=0, keepdims=True)
        return acc + jnp.where(down == mine.astype(jnp.int32), rate_ref[r], 0.0)

    acc = lax.fori_loop(0, 16, entry, jnp.zeros((DEVICES, DEVICES), jnp.float32))
    first_sum = jnp.sum(acc.T, axis=0, keepdims=True)
    part0[...] = first_sum
    to_me = jnp.where(owner == me, jnp.bitwise_and(slots, 127), 0).astype(jnp.float32)
    slot_out_ref[...] = jnp.sum(to_me.T, axis=0, keepdims=True).astype(jnp.int32)

    tell(part0, row0, 7, twin)
    wait(row0, small_got.at[7])
    first_sum = part0[...] + row0[...]
    part1[...] = first_sum
    row1[pl.ds(y, 1), :] = first_sum
    forward2(AWAY[0])
    tell(part1, row1.at[pl.ds(y, 1)], 3, ys)
    for second in AWAY[1:]:
        forward2(second)
    wait(row1.at[pl.ds(0, 3)], small_got.at[3])
    second_sum = jnp.sum(row1[...], axis=0, keepdims=True)
    part2[...] = second_sum
    row2[pl.ds(z, 1), :] = second_sum
    for g in range(3):
        phase3((g, 0, 0))
    tell(part2, row2.at[pl.ds(z, 1)], 4, zs)
    for first in AWAY:
        for g in range(3):
            key = (g, first, 0)
            wait(mid1.at[span(key)], got1.at[spot(key)])
            phase3(key)
    for second in AWAY:
        for g in range(3):
            key = (g, 0, second)
            wait(mid2.at[span(key)], got2.at[spot(key)])
            phase3(key)
    for second in AWAY:
        if second == LATE_SUM:
            wait(row2.at[pl.ds(0, 3)], small_got.at[4])
            third_sum = jnp.sum(row2[...], axis=0, keepdims=True)
            part3[...] = third_sum
            row3[pl.ds(x, 1), :] = third_sum
        for first in AWAY:
            for g in range(3):
                key = (g, first, second)
                wait(mid2.at[span(key)], got2.at[spot(key)])
                phase3(key)
            if second == LATE_SUM and first == 2:
                tell(part3, row3.at[pl.ds(x, 1)], 5, xs)
    wait(row3.at[pl.ds(0, 3)], small_got.at[5])
    load_ref[...] = jnp.sum(row3[...], axis=0, keepdims=True) * (1.0 / 2048.0)

    pages = [sum(len(v) for k, v in CHUNKS.items() if k[i]) for i in (1, 2)]
    far = sum(1 for v in CHUNKS.values() for _, s, k in v if s or k)
    wait(send_ref.at[pl.ds(0, pages[0])], sent.at[0])
    wait(send_ref.at[pl.ds(0, pages[1])], sent.at[1])
    wait(send_ref.at[pl.ds(0, far)], sent.at[2])
    wait(pages_ref.at[pl.ds(0, far)], got3)
    wait(pages_ref.at[pl.ds(0, DEVICES - far)], local.at[1])
    wait(known.at[0, 0, pl.ds(0, 3)], small_sent.at[0])
    wait(known.at[0, 0, pl.ds(0, 12)], small_sent.at[1])
    wait(known.at[0, pl.ds(0, 3)], small_sent.at[2])
    wait(known.at[0], small_sent.at[6])
    wait(row0, small_sent.at[7])
    wait(row1.at[pl.ds(0, 3)], small_sent.at[3])
    wait(row2.at[pl.ds(0, 3)], small_sent.at[4])
    wait(row3.at[pl.ds(0, 3)], small_sent.at[5])


SMEM = pl.BlockSpec(memory_space=pltpu.SMEM)
VMEM = pl.BlockSpec(memory_space=pltpu.VMEM)
HBM = pl.BlockSpec(memory_space=pltpu.HBM)


def on_device(kv_pages, new_slot, request_rate, page_table):
    block = jax.ShapeDtypeStruct((DEVICES,) + kv_pages.shape[2:], kv_pages.dtype)
    buffer = pltpu.VMEM(block.shape, block.dtype)
    line = lambda dtype: jax.ShapeDtypeStruct((1, DEVICES), dtype)
    row = lambda n, dtype=jnp.float32: pltpu.VMEM((n, DEVICES), dtype)
    dma = pltpu.SemaphoreType.DMA
    arrived, slot, total = pl.pallas_call(
        exchange_kernel,
        out_shape=(block, line(jnp.int32), line(jnp.float32)),
        in_specs=[HBM] * 4,
        out_specs=(VMEM, VMEM, VMEM),
        scratch_shapes=[
            pltpu.SMEM((16,), jnp.float32), row(16, jnp.int32), row(1, jnp.int32),
            buffer, buffer, buffer, buffer, row(1, jnp.int32), pltpu.SMEM((1, DEVICES), jnp.int32),
            pltpu.VMEM((2, 4, 16, DEVICES), jnp.int32),
            row(1), row(4), row(4), row(4), row(1), row(1), row(1), row(1),
            dma((3,)), dma((48,)), dma((48,)), dma, dma((7,)), dma((8,)), dma((8,)),
        ],
        compiler_params=pltpu.CompilerParams(
            collective_id=0, has_side_effects=True, vmem_limit_bytes=36 << 20
        ),
        name="exchange",
    )(*(pltpu.with_memory_space_constraint(v, pltpu.HBM)
        for v in (request_rate, page_table, new_slot.reshape(1, DEVICES), kv_pages)))
    migrated, load = pl.pallas_call(
        place_kernel,
        out_shape=(jax.ShapeDtypeStruct(kv_pages.shape, kv_pages.dtype), line(jnp.float32)),
        in_specs=[VMEM, VMEM, VMEM],
        out_specs=(HBM, HBM),
        scratch_shapes=[
            pltpu.SMEM((1, DEVICES), jnp.int32), pltpu.SMEM((DEVICES,), jnp.int32), dma((3,)),
        ],
        compiler_params=pltpu.CompilerParams(vmem_limit_bytes=12 << 20),
        name="place",
    )(slot, total, arrived)
    return migrated, load.reshape(DEVICES)


def solution(mesh):
    split = Mesh(mesh.devices.reshape(4, 4, 2, mesh.shape["dev"]), AXES)
    placed = (P(AXES, None, None, None, None), P(AXES), P(AXES), P(AXES, None))
    return jax.shard_map(
        on_device,
        mesh=split,
        in_specs=placed,
        out_specs=(P(AXES, None, None, None, None), P()),
        check_vma=False,
    )
```
